32 devices in a mesh: dp: 8 (over z, x), cls: 4 (over y, core).
Axes of the slice: x: 2, y: 2, z: 4, core: 2. Of those that a mesh axis runs over, the one named last changes fastest.
Arguments:
- embeddings: bfloat16 [24576, 768], P('dp'), may hold values from -6 to 6
- labels: int32 [24576], P('dp'), may hold values from 0 to 2751, as said below
- row_count: int32 [8], P('dp'), may hold values from 768 to 3072
Outputs:
- class_means: float32 [2752, 768], P(('dp', 'cls'))
- prototypes: float32 [2752, 768], P(('dp', 'cls'))
- similarity: float32 [24576], P('dp')
The draws below stay inside these ranges and needn't reach their ends.
Inputs may be any that keep to these rules, and one draw needn't show every extreme that they name: Rows of index i of dp at or beyond row_count[i] are padding. `labels`: classes c and c' belong to the same block when c // 86 == c' // 86; block b belongs to index b mod 4 of cls. The rows of one index of dp name at most 16 distinct classes of any one block. Some block has exactly 16 of its classes named by the rows of every index of dp. The rows of some index of dp name exactly 16 classes of every block of some index of cls.
All inputs are finite; a program needn't handle non-finite values.
Results may differ from the reference program's by a relative error of at most 0.0017.
Values sent between devices are 32-bit elements; how exact they have to be, the bound alone decides.
A program may use at most 64 MiB of HBM per device.

```python
import jax
import jax.numpy as jnp
from jax import lax

D = 768
CLS_DEV = 86
SLOTS = 16
ROWS_DEV = 3072
CLASSES = 2752
ROWS = 24576
N_DP = 8


def draw_labels(key, part):
    blocks = ROWS // ROWS_DEV
    owners = CLASSES // CLS_DEV
    group_count = owners // blocks
    keys = jax.random.split(jax.random.fold_in(key, 17), 7)
    class_iota = jnp.arange(CLS_DEV, dtype=jnp.int32)
    scores = jax.random.randint(keys[0], (blocks, owners, CLS_DEV), 0, 1 << 20) * CLS_DEV + class_iota
    allowed = jnp.argsort(scores, axis=2)[:, :, :SLOTS].astype(jnp.int32)
    owner_scores = jax.random.randint(keys[1], (owners,), 0, 1 << 20) * owners + jnp.arange(owners, dtype=jnp.int32)
    owner_order = jnp.argsort(owner_scores).astype(jnp.int32)
    first_pick = jax.random.randint(keys[2], (blocks, ROWS_DEV), 0, owners)
    second_pick = jax.random.randint(keys[3], (blocks, ROWS_DEV), 0, owners)
    owner_rank = jnp.minimum(first_pick, second_pick).astype(jnp.int32)
    slot_first = jax.random.randint(keys[4], (blocks, ROWS_DEV), 0, SLOTS)
    slot_second = jax.random.randint(keys[5], (blocks, ROWS_DEV), 0, SLOTS)
    slot = jnp.minimum(slot_first, slot_second).astype(jnp.int32)
    position = jnp.broadcast_to(jnp.arange(ROWS_DEV, dtype=jnp.int32)[None, :], (blocks, ROWS_DEV))
    block_index = jnp.broadcast_to(jnp.arange(blocks, dtype=jnp.int32)[:, None], (blocks, ROWS_DEV))
    forced = position < SLOTS
    owner_rank = jnp.where(forced, 0, owner_rank)
    slot = jnp.where(forced, position, slot)
    chosen_owner = owner_order[owner_rank].astype(jnp.int32)
    full_sender = jax.random.randint(keys[6], (), 0, blocks).astype(jnp.int32)
    base_group = (owner_order[0] % group_count).astype(jnp.int32)
    widened = (block_index == full_sender) & (position < blocks * SLOTS)
    wide_owner = (base_group + group_count * (position // SLOTS)).astype(jnp.int32)
    chosen_owner = jnp.where(widened, wide_owner, chosen_owner).astype(jnp.int32)
    slot = jnp.where(widened, position % SLOTS, slot).astype(jnp.int32)
    local_class = allowed[block_index, chosen_owner, slot]
    labels = chosen_owner * CLS_DEV + local_class
    return labels.reshape(ROWS).astype(jnp.int32)


def set_ends(entries, key, smallest, largest):
    place = [jax.random.randint(jax.random.fold_in(key, axis), (), 0, length) for axis, length in enumerate(entries.shape)]
    widest = entries.shape.index(max(entries.shape))
    neighbour = place[:widest] + [(place[widest] + 1) % entries.shape[widest]] + place[widest + 1:]
    return entries.at[tuple(place)].set(smallest).at[tuple(neighbour)].set(largest)


def level_of(stream_key, shape, cuts, smallest, top_value):
    gain, own = 1.0, jax.random.fold_in(stream_key, 6)
    for axis_at, shards_of in cuts:
        heights = jnp.exp(jax.random.uniform(jax.random.fold_in(own, axis_at), (shards_of,), jnp.float32, smallest / len(cuts), top_value / len(cuts)))
        gain = gain * jnp.repeat(heights, shape[axis_at] // shards_of).reshape([-1 if axis == axis_at else 1 for axis in range(len(shape))])
    return gain


def bell_draw(rng, extent, deviation, reach, cuts=(), held_as=jnp.bfloat16):
    array = jax.random.normal(rng, extent, jnp.float32) * deviation
    if len(cuts) > 0:
        array = level_of(rng, extent, cuts, -0.22, 0.18) * array
    return jnp.clip(array, min=-reach, max=reach).astype(held_as)


def setup_inputs(seed: int = 0) -> dict:
    splits = jax.random.split(jax.random.key(seed), 4)
    embeddings = bell_draw(splits[0], (ROWS, D), 1.0, 6.0, ((0, 8),))
    labels = draw_labels(jax.random.fold_in(splits[3], 71), 0)
    row_count = set_ends(jax.random.randint(splits[2], (N_DP,), max(ROWS_DEV // 4, N_DP * SLOTS), ROWS_DEV + 1), jax.random.fold_in(splits[2], 1), max(ROWS_DEV // 4, N_DP * SLOTS), ROWS_DEV).astype(jnp.int32)
    return dict(embeddings=embeddings, labels=labels, row_count=row_count)


epsilon = 1e-06
sharpness = 4.0

def normalize(matrix):
    return matrix / jnp.sqrt(lax.optimization_barrier(jnp.sum(matrix * matrix, axis=1, keepdims=True)) + epsilon)

def reference(embeddings, labels, row_count):
    row_total = embeddings.shape[0]
    position = jnp.arange(row_total, dtype=jnp.int32)
    owner = (position // ROWS_DEV).astype(jnp.int32)
    alive = (position % ROWS_DEV < row_count[owner]).astype(jnp.float32)
    features = embeddings.astype(jnp.float32)
    class_sums = jax.ops.segment_sum(features * alive[:, None], labels, num_segments=CLASSES)
    counts = jax.ops.segment_sum(alive, labels, num_segments=CLASSES)
    class_means = class_sums / jnp.maximum(counts, 1.0)[:, None]
    unit_rows = normalize(class_means)
    lengths = jnp.sqrt(lax.optimization_barrier(jnp.sum(features * features, axis=1)) + epsilon)
    similarity = alive * lax.optimization_barrier(jnp.sum(features * unit_rows[labels], axis=1)) / lengths
    weight = (alive * jnp.exp(sharpness * (similarity - 1.0))).astype(jnp.bfloat16).astype(jnp.float32)
    weighted = jax.ops.segment_sum(features * weight[:, None], labels, num_segments=CLASSES)
    prototypes = normalize(weighted)
    return (class_means, prototypes, similarity)
```

```python
import functools

import jax
import jax.numpy as jnp
from jax import lax
from jax.experimental import pallas as pl
from jax.experimental.pallas import tpu as pltpu
from jax.sharding import PartitionSpec as P

CLS_DEV = 86
SLOTS = 16
CLS_PAD = 128
CHUNK = 384
ROW_TILE = 512

epsilon = 1e-06
sharpness = 4.0

f32 = jnp.float32
bf16 = jnp.bfloat16
NN = (((1,), (0,)), ((), ()))
NT = (((1,), (1,)), ((), ()))


def dot(a, b, dims=NN):
    return lax.dot_general(a, b, dims, preferred_element_type=f32)


def split(x):
    hi = x.astype(bf16)
    return hi, (x - hi.astype(f32)).astype(bf16)


def iota(shape, dim):
    return lax.broadcasted_iota(jnp.int32, shape, dim).astype(f32)


def kernel(
    n,
    m,
    count_ref,
    label_ref,
    emb_ref,
    means_ref,
    proto_ref,
    sim_ref,
    label_rows,
    emb,
    onehot,
    weighted_onehot,
    place_t,
    cnt_send,
    cnt_recv,
    a_send,
    a_recv,
    b_send,
    b_recv,
    c_send,
    c_recv,
    s_send,
    s_recv,
    dot_row,
    len_row,
    own,
    label_sem,
    load_sem,
    cnt_ss,
    cnt_rs,
    big_ss,
    big_rs,
    s_ss,
    s_rs,
):
    rows = label_ref.shape[1]
    chunks = emb.shape[0]
    slots = n * SLOTS
    me = lax.axis_index("dp")
    mine = lax.axis_index("cls")
    half = n // 2
    height = half * SLOTS

    def index_of(g, z):
        return 2 * z + lax.rem(g + z, 2)

    my_z = me // 2
    my_position = lax.rem(my_z + me, 2) * half + my_z

    def partners(g):
        for off in range(half):
            z = lax.rem(my_z + off, half)
            yield index_of(g, z), g * half + z

    label_load = pltpu.make_async_copy(label_ref, label_rows, label_sem)
    label_load.start()
    loads = []
    for f in range(chunks):
        load = pltpu.make_async_copy(
            emb_ref.at[:, pl.ds(f * CHUNK, CHUNK)], emb.at[f], load_sem.at[f]
        )
        load.start()
        loads.append(load)

    barrier = pltpu.get_barrier_semaphore()
    for off in range(1, n):
        pl.semaphore_signal(
            barrier, inc=1, device_id={"dp": lax.rem(me + off, n)}, device_id_type=pl.DeviceIdType.MESH
        )
    for off in range(1, m):
        pl.semaphore_signal(
            barrier, inc=1, device_id={"cls": lax.rem(mine + off, m)}, device_id_type=pl.DeviceIdType.MESH
        )

    label_load.wait()
    label = label_rows[...].astype(f32)
    block = jnp.floor((label + 0.5) * (1.0 / CLS_DEV))
    place = label - CLS_DEV * block
    owner = jnp.floor((block + 0.5) * (1.0 / m))
    group = block - m * owner
    pair = jnp.floor(owner * 0.5)
    odd = pair + owner - 2.0 * jnp.floor((pair + owner) * 0.5)
    owner = odd * half + pair
    alive = lax.broadcasted_iota(jnp.int32, (1, rows), 1) < count_ref[0]
    owned = (group == mine.astype(f32)) & alive
    place = jnp.where(owned, place, -1.0)
    owner = jnp.where(owned, owner, -1.0)

    owner_mask = iota((n, rows), 0) == owner
    place_hot = jnp.where(iota((CLS_PAD, rows), 0) == place, 1.0, 0.0).astype(bf16)
    counts = dot(jnp.where(owner_mask, 1.0, 0.0).astype(bf16), place_hot, NT)
    upper = jnp.where(
        iota((CLS_PAD, CLS_PAD), 0) <= iota((CLS_PAD, CLS_PAD), 1), 1.0, 0.0
    ).astype(bf16)

    def ranks(table):
        return dot(jnp.where(table > 0, 1.0, 0.0).astype(bf16), upper) - 1.0

    for o in range(n):
        cnt_send[o] = jnp.broadcast_to(counts[o : o + 1, :], (8, CLS_PAD))
    cnt_recv[my_position] = cnt_send[my_position]

    rank_of = dot(ranks(counts).astype(bf16), place_hot) + SLOTS * iota((n, rows), 0)
    slot = jnp.sum(jnp.where(owner_mask, rank_of, 0.0), axis=0, keepdims=True)
    slot = jnp.where(owned, slot, -1.0)
    onehot[...] = jnp.where(iota((slots, rows), 0) == slot, 1.0, 0.0).astype(bf16)

    pl.semaphore_wait(barrier, n - 1 + m - 1)

    def dp_copy(src, dst, send_sem, recv_sem, target):
        return pltpu.make_async_remote_copy(
            src_ref=src,
            dst_ref=dst,
            send_sem=send_sem,
            recv_sem=recv_sem,
            device_id={"dp": target},
            device_id_type=pl.DeviceIdType.MESH,
        )

    def cnt_copy(target, to, frm):
        return dp_copy(cnt_send.at[to], cnt_recv.at[frm], cnt_ss.at[to], cnt_rs.at[frm], target)

    buffers = ((a_send, a_recv), (b_send, b_recv), (c_send, c_recv))

    def big_copy(phase, f, target, to, frm):
        send, recv = buffers[phase]
        return dp_copy(
            send.at[f, to], recv.at[f, frm], big_ss.at[phase, f, to], big_rs.at[phase, f, frm], target
        )

    def others(g, action):
        for target, to in partners(g):
            pl.when(target != me)(functools.partial(action, target, to))

    def send(phase, f, g):
        others(g, lambda target, to: big_copy(phase, f, target, to, my_position).start())

    def keep(phase, f):
        out, recv = buffers[phase]
        recv[f, my_position] = out[f, my_position]

    def arrived(phase, f, first, count):
        for p in range(first, first + count):
            pl.when(p != my_position)(lambda: big_copy(phase, f, me, p, p).wait_recv())
        recv = buffers[phase][1]
        return recv[f, first : first + count].reshape(count * SLOTS, CHUNK)

    for g in range(2):
        others(g, lambda target, to: cnt_copy(target, to, my_position).start())

    for f in range(chunks):
        loads[f].wait()
        a_send[f] = dot(onehot[...], emb[f]).reshape(n, SLOTS, CHUNK)
        send(0, f, 0)
        keep(0, f)
    for f in range(chunks):
        send(0, f, 1)

    for t in range(0, rows, ROW_TILE):
        squares = jnp.zeros((ROW_TILE, 128), f32)
        for f in range(chunks):
            for k in range(0, CHUNK, 128):
                x = emb[f, t : t + ROW_TILE, k : k + 128].astype(f32)
                squares = squares + x * x
        total = jnp.sum(jnp.transpose(squares), axis=0, keepdims=True)
        len_row[:, t : t + ROW_TILE] = jnp.sqrt(total + epsilon)

    for p in range(n):
        pl.when(p != my_position)(lambda: cnt_copy(me, p, p).wait_recv())
    table = jnp.concatenate([cnt_recv[i, 0:1, :] for i in range(n)], axis=0)
    table_rank = jnp.where(table > 0, ranks(table), -1.0)
    slot_iota = iota((SLOTS, CLS_PAD), 0)
    for i in range(n):
        place_t[i * SLOTS : (i + 1) * SLOTS, :] = jnp.where(
            table_rank[i : i + 1, :] == slot_iota, 1.0, 0.0
        )
    to_slots = place_t[...].astype(bf16)
    to_classes = jnp.transpose(place_t[...]).astype(bf16)
    own_counts = jnp.maximum(jnp.sum(table, axis=0, keepdims=True), 1.0)
    divisor = jnp.transpose(jnp.broadcast_to(own_counts, (CLS_PAD, CLS_PAD)))[:, 0:1]

    for f in range(chunks):
        hi, lo = split(arrived(0, f, 0, n))
        means = (dot(to_classes, hi) + dot(to_classes, lo)) / divisor
        hi, lo = split(means)
        b_send[f] = (dot(to_slots, hi) + dot(to_slots, lo)).reshape(n, SLOTS, CHUNK)
        send(1, f, 0)
        send(1, f, 1)
        keep(1, f)
        means_ref[:, f * CHUNK : (f + 1) * CHUNK] = means[:CLS_DEV, :]

    for g in range(2):
        span = slice(g * height, (g + 1) * height)
        norm = jnp.zeros((height, 1), f32)
        for f in range(chunks):
            mean = arrived(1, f, g * half, half)
            norm = norm + jnp.sum(mean * mean, axis=1, keepdims=True)
            both = jnp.concatenate(split(mean), axis=0)
            for t in range(0, rows, ROW_TILE):
                cols = slice(t, t + ROW_TILE)
                product = dot(both, emb[f, cols, :], NT)
                product = product[:height, :] + product[height:, :]
                product = jnp.sum(
                    product * onehot[span, cols].astype(f32), axis=0, keepdims=True
                )
                dot_row[:, cols] = product if f == 0 else dot_row[:, cols] + product
        scale = 1.0 / jnp.sqrt(norm + epsilon)
        for t in range(0, rows, ROW_TILE):
            cols = slice(t, t + ROW_TILE)
            hot = onehot[span, cols].astype(f32)
            row_scale = jnp.sum(hot * scale, axis=0, keepdims=True)
            similarity = dot_row[:, cols] * row_scale / len_row[:, cols]
            s_send[:, cols] = similarity if g == 0 else s_send[:, cols] + similarity
            weight = jnp.exp(sharpness * (similarity - 1.0))
            weighted_onehot[:, cols] = (hot * weight).astype(bf16)
        for f in range(chunks):
            c_send[f, g * half : (g + 1) * half] = dot(weighted_onehot[...], emb[f]).reshape(
                half, SLOTS, CHUNK
            )
            send(2, f, g)
    for f in range(chunks):
        keep(2, f)

    def s_copy(off):
        return pltpu.make_async_remote_copy(
            src_ref=s_send,
            dst_ref=s_recv.at[mine],
            send_sem=s_ss.at[off - 1],
            recv_sem=s_rs.at[off - 1],
            device_id={"cls": lax.rem(mine + off, m)},
            device_id_type=pl.DeviceIdType.MESH,
        )

    for off in range(1, m):
        s_copy(off).start()
    s_recv[mine] = s_send[...]
    for off in range(1, m):
        s_copy(off).wait_recv()
    full = s_recv[0]
    for j in range(1, m):
        full = full + s_recv[j]
    sim_ref[...] = full

    norm = jnp.zeros((CLS_PAD, 1), f32)
    for f in range(chunks):
        hi, lo = split(arrived(2, f, 0, n))
        part = dot(to_classes, hi) + dot(to_classes, lo)
        own[f] = part
        norm = norm + jnp.sum(part * part, axis=1, keepdims=True)
    length = jnp.sqrt(norm + epsilon)
    for f in range(chunks):
        proto_ref[:, f * CHUNK : (f + 1) * CHUNK] = (own[f] / length)[:CLS_DEV, :]

    def sent(target, to):
        cnt_copy(target, to, my_position).wait_send()
        for phase in range(3):
            for f in range(chunks):
                big_copy(phase, f, target, to, my_position).wait_send()

    for g in range(2):
        others(g, sent)
    for off in range(1, m):
        s_copy(off).wait_send()


def finish(means_ref, proto_ref, sim_ref, means_out, proto_out, sim_out, sems):
    copies = [
        pltpu.make_async_copy(means_ref, means_out, sems.at[0]),
        pltpu.make_async_copy(proto_ref, proto_out, sems.at[1]),
        pltpu.make_async_copy(sim_ref, sim_out, sems.at[2]),
    ]
    for copy in copies:
        copy.start()
    for copy in copies:
        copy.wait()


def shards(embeddings, labels, row_count):
    rows, width = embeddings.shape
    n = lax.axis_size("dp")
    m = lax.axis_size("cls")
    chunks = width // CHUNK
    slots = n * SLOTS
    vmem = pl.BlockSpec(memory_space=pltpu.VMEM)
    anywhere = pl.BlockSpec(memory_space=pl.ANY)
    exchange_buffer = pltpu.VMEM((chunks, n, SLOTS, CHUNK), f32)
    dma = pltpu.SemaphoreType.DMA
    results = (
        jax.ShapeDtypeStruct((CLS_DEV, width), f32),
        jax.ShapeDtypeStruct((CLS_DEV, width), f32),
        jax.ShapeDtypeStruct((1, rows), f32),
    )
    held = pl.pallas_call(
        functools.partial(kernel, n, m),
        out_shape=results,
        in_specs=[
            pl.BlockSpec(memory_space=pltpu.SMEM),
            pl.BlockSpec(memory_space=pltpu.HBM),
            pl.BlockSpec(memory_space=pltpu.HBM),
        ],
        out_specs=(vmem, vmem, vmem),
        scratch_shapes=[
            pltpu.VMEM((1, rows), jnp.int32),
            pltpu.VMEM((chunks, rows, CHUNK), bf16),
            pltpu.VMEM((slots, rows), bf16),
            pltpu.VMEM((slots // 2, rows), bf16),
            pltpu.VMEM((slots, CLS_PAD), f32),
            pltpu.VMEM((n, 8, CLS_PAD), f32),
            pltpu.VMEM((n, 8, CLS_PAD), f32),
            exchange_buffer,
            exchange_buffer,
            exchange_buffer,
            exchange_buffer,
            exchange_buffer,
            exchange_buffer,
            pltpu.VMEM((1, rows), f32),
            pltpu.VMEM((m, 1, rows), f32),
            pltpu.VMEM((1, rows), f32),
            pltpu.VMEM((1, rows), f32),
            pltpu.VMEM((chunks, CLS_PAD, CHUNK), f32),
            dma,
            dma((chunks,)),
            dma((n,)),
            dma((n,)),
            dma((3, chunks, n)),
            dma((3, chunks, n)),
            dma((m - 1,)),
            dma((m - 1,)),
        ],
        compiler_params=pltpu.CompilerParams(
            collective_id=0, has_side_effects=True, vmem_limit_bytes=32 * 1024 * 1024
        ),
    )(
        row_count,
        pltpu.with_memory_space_constraint(labels.reshape(1, rows), pltpu.HBM),
        pltpu.with_memory_space_constraint(embeddings, pltpu.HBM),
    )
    means, protos, similarity = pl.pallas_call(
        finish,
        out_shape=results,
        in_specs=[anywhere] * 3,
        out_specs=(anywhere,) * 3,
        scratch_shapes=[pltpu.SemaphoreType.DMA((3,))],
        compiler_params=pltpu.CompilerParams(vmem_limit_bytes=1024 * 1024),
    )(*held)
    return (means, protos, similarity.reshape(rows))


def solution(mesh):
    in_specs = (P("dp", None), P("dp"), P("dp"))
    out_specs = (P(("dp", "cls"), None), P(("dp", "cls"), None), P("dp"))
    return jax.shard_map(shards, mesh=mesh, in_specs=in_specs, out_specs=out_specs, check_vma=False)
```

```python
import functools

import jax
import jax.numpy as jnp
from jax import lax
from jax.experimental import pallas as pl
from jax.experimental.pallas import tpu as pltpu
from jax.sharding import PartitionSpec as P

CLS_DEV = 86
SLOTS = 16
CLS_PAD = 128
CHUNK = 384
ROW_TILE = 512

epsilon = 1e-06
sharpness = 4.0

f32 = jnp.float32
bf16 = jnp.bfloat16
NN = (((1,), (0,)), ((), ()))
NT = (((1,), (1,)), ((), ()))


def dot(a, b, dims=NN):
    return lax.dot_general(a, b, dims, preferred_element_type=f32)


def split(x):
    hi = x.astype(bf16)
    return hi, (x - hi.astype(f32)).astype(bf16)


def iota(shape, dim):
    return lax.broadcasted_iota(jnp.int32, shape, dim).astype(f32)


def plan(n):
    half = n // 2
    cut = max(1, half // 4)
    items = list(range(half)) + sorted(range(half, n), key=lambda k: (-(k // 2), k % 2))
    groups = [(0, half + cut), (half + cut, half + 2 * cut), (half + 2 * cut, n)]
    order = [half - 1] + list(range(half, n - 1)) + list(range(1, half - 1)) + [n - 1]
    return items, groups, order


def kernel(
    n,
    m,
    count_hbm,
    label_ref,
    emb_ref,
    means_out,
    proto_out,
    sim_out,
    count_ref,
    means_ref,
    proto_ref,
    sim_ref,
    label_rows,
    emb,
    onehot,
    weighted_onehot,
    place_t,
    cnt_send,
    cnt_recv,
    a_send,
    a_recv,
    b_send,
    b_recv,
    c_send,
    c_recv,
    s_send,
    s_recv,
    dot_row,
    len_row,
    own,
    out_sems,
    count_sem,
    label_sem,
    load_sem,
    cnt_ss,
    cnt_rs,
    big_ss,
    big_rs,
    s_ss,
    s_rs,
):
    rows = label_ref.shape[1]
    chunks = emb.shape[0]
    slots = n * SLOTS
    me = lax.axis_index("dp")
    mine = lax.axis_index("cls")
    items, groups, order = plan(n)

    def partner(p):
        target, bit = me, 1
        while bit < n:
            if items[p] & bit:
                target = target + bit - 2 * bit * lax.rem(lax.div(me, bit), 2)
            bit *= 2
        return target

    label_load = pltpu.make_async_copy(label_ref, label_rows, label_sem)
    label_load.start()
    count_load = pltpu.make_async_copy(count_hbm, count_ref, count_sem)
    count_load.start()
    barrier = pltpu.get_barrier_semaphore()
    for p in range(1, n):
        pl.semaphore_signal(
            barrier, inc=1, device_id={"dp": partner(p)}, device_id_type=pl.DeviceIdType.MESH
        )
    for off in range(1, m):
        pl.semaphore_signal(
            barrier, inc=1, device_id={"cls": lax.rem(mine + off, m)}, device_id_type=pl.DeviceIdType.MESH
        )
    loads = []
    for f in range(chunks):
        load = pltpu.make_async_copy(
            emb_ref.at[:, pl.ds(f * CHUNK, CHUNK)], emb.at[f], load_sem.at[f]
        )
        load.start()
        loads.append(load)

    position = lax.broadcasted_iota(jnp.int32, (n, rows), 0)
    peers = jnp.zeros((n, rows), f32)
    for p in range(n):
        peers = jnp.where(position == p, partner(p).astype(f32), peers)

    count_load.wait()
    label_load.wait()
    label = label_rows[...].astype(f32)
    block = jnp.floor((label + 0.5) * (1.0 / CLS_DEV))
    place = label - CLS_DEV * block
    owner = jnp.floor((block + 0.5) * (1.0 / m))
    group = block - m * owner
    alive = lax.broadcasted_iota(jnp.int32, (1, rows), 1) < count_ref[0]
    owned = (group == mine.astype(f32)) & alive
    place = jnp.where(owned, place, -1.0)
    owner = jnp.where(owned, owner, -1.0)

    owner_mask = peers == owner
    place_hot = jnp.where(iota((CLS_PAD, rows), 0) == place, 1.0, 0.0).astype(bf16)
    counts = dot(jnp.where(owner_mask, 1.0, 0.0).astype(bf16), place_hot, NT)
    upper = jnp.where(
        iota((CLS_PAD, CLS_PAD), 0) <= iota((CLS_PAD, CLS_PAD), 1), 1.0, 0.0
    ).astype(bf16)

    def ranks(table):
        return dot(jnp.where(table > 0, 1.0, 0.0).astype(bf16), upper) - 1.0

    for p in range(n):
        cnt_send[p] = counts[p : p + 1, :]
    cnt_recv[0] = cnt_send[0]

    rank_of = dot(ranks(counts).astype(bf16), place_hot) + SLOTS * iota((n, rows), 0)
    slot = jnp.sum(jnp.where(owner_mask, rank_of, 0.0), axis=0, keepdims=True)
    slot = jnp.where(owned, slot, -1.0)
    onehot[...] = jnp.where(iota((slots, rows), 0) == slot, 1.0, 0.0).astype(bf16)

    def dp_copy(p, src, dst, send_sem, recv_sem):
        return pltpu.make_async_remote_copy(
            src_ref=src,
            dst_ref=dst,
            send_sem=send_sem,
            recv_sem=recv_sem,
            device_id={"dp": partner(p)},
            device_id_type=pl.DeviceIdType.MESH,
        )

    def cnt_copy(p, count=1):
        span = pl.ds(p, count)
        return dp_copy(p, cnt_send.at[span], cnt_recv.at[span], cnt_ss, cnt_rs)

    buffers = ((a_send, a_recv), (b_send, b_recv), (c_send, c_recv))

    def big_copy(phase, f, p, g=0):
        out, recv = buffers[phase]
        return dp_copy(p, out.at[f, p], recv.at[f, p], big_ss.at[phase], big_rs.at[phase, f, g])

    def piece(phase, f, g, first, stop):
        out, recv = buffers[phase]
        span = pl.ds(max(first, 1), stop - max(first, 1))
        return dp_copy(
            max(first, 1), out.at[f, span], recv.at[f, span], big_ss.at[phase], big_rs.at[phase, f, g]
        )

    def send(phase, f, positions, g=0):
        for p in positions:
            if p > 0:
                big_copy(phase, f, p, g).start()

    def keep(phase, f):
        out, recv = buffers[phase]
        recv[f, 0] = out[f, 0]

    def arrived(phase, f, g=0, first=0, stop=n):
        piece(phase, f, g, first, stop).wait_recv()
        return buffers[phase][1][f, first:stop].reshape((stop - first) * SLOTS, CHUNK)

    loads[0].wait()
    a_send[0] = dot(onehot[...], emb[0]).reshape(n, SLOTS, CHUNK)
    pl.semaphore_wait(barrier, n - 1 + m - 1)
    for p in order:
        cnt_copy(p).start()
    send(0, 0, order)
    keep(0, 0)
    for f in range(1, chunks):
        loads[f].wait()
        a_send[f] = dot(onehot[...], emb[f]).reshape(n, SLOTS, CHUNK)
        send(0, f, order)
        keep(0, f)

    for t in range(0, rows, ROW_TILE):
        squares = jnp.zeros((ROW_TILE, 128), f32)
        for f in range(chunks):
            for k in range(0, CHUNK, 128):
                x = emb[f, t : t + ROW_TILE, k : k + 128].astype(f32)
                squares = squares + x * x
        total = jnp.sum(jnp.transpose(squares), axis=0, keepdims=True)
        len_row[:, t : t + ROW_TILE] = jnp.sqrt(total + epsilon)

    cnt_copy(1, n - 1).wait_recv()
    table = jnp.concatenate([cnt_recv[p] for p in range(n)], axis=0)
    table_rank = jnp.where(table > 0, ranks(table), -1.0)
    slot_iota = iota((SLOTS, CLS_PAD), 0)
    for p in range(n):
        place_t[p * SLOTS : (p + 1) * SLOTS, :] = jnp.where(
            table_rank[p : p + 1, :] == slot_iota, 1.0, 0.0
        )
    to_slots = place_t[...].astype(bf16)
    to_classes = jnp.transpose(place_t[...]).astype(bf16)
    own_counts = jnp.maximum(jnp.sum(table, axis=0, keepdims=True), 1.0)
    divisor = jnp.transpose(jnp.broadcast_to(own_counts, (CLS_PAD, CLS_PAD)))[:, 0:1]

    for f in range(chunks):
        hi, lo = split(arrived(0, f))
        means = (dot(to_classes, hi) + dot(to_classes, lo)) / divisor
        hi, lo = split(means)
        b_send[f] = (dot(to_slots, hi) + dot(to_slots, lo)).reshape(n, SLOTS, CHUNK)
        for g, (first, stop) in enumerate(groups):
            send(1, f, [p for p in order if first <= p < stop], g)
        keep(1, f)
        means_ref[:, f * CHUNK : (f + 1) * CHUNK] = means[:CLS_DEV, :]
    means_copy = pltpu.make_async_copy(means_ref, means_out, out_sems.at[0])
    means_copy.start()

    def project(f, g, first, stop, start):
        mean = arrived(1, f, g, first, stop)
        height = (stop - first) * SLOTS
        both = jnp.concatenate(split(mean), axis=0)
        for t in range(0, rows, ROW_TILE):
            cols = slice(t, t + ROW_TILE)
            product = dot(both, emb[f, cols, :], NT)
            product = product[:height, :] + product[height:, :]
            hot = onehot[first * SLOTS : stop * SLOTS, cols].astype(f32)
            product = jnp.sum(product * hot, axis=0, keepdims=True)
            dot_row[:, cols] = product if start else dot_row[:, cols] + product
        return jnp.sum(mean * mean, axis=1, keepdims=True)

    norms = [0.0] * len(groups)
    for f in range(chunks - 1):
        for g, (first, stop) in enumerate(groups):
            norms[g] = norms[g] + project(f, g, first, stop, f == 0 and g == 0)
    for g, (first, stop) in enumerate(groups):
        span = slice(first * SLOTS, stop * SLOTS)
        norm = norms[g] + project(chunks - 1, g, first, stop, chunks == 1 and g == 0)
        scale = 1.0 / jnp.sqrt(norm + epsilon)
        for t in range(0, rows, ROW_TILE):
            cols = slice(t, t + ROW_TILE)
            hot = onehot[span, cols].astype(f32)
            row_scale = jnp.sum(hot * scale, axis=0, keepdims=True)
            similarity = dot_row[:, cols] * row_scale / len_row[:, cols]
            s_send[:, cols] = similarity if g == 0 else s_send[:, cols] + similarity
            weight = jnp.exp(sharpness * (similarity - 1.0))
            weighted_onehot[span, cols] = (hot * weight).astype(bf16)
        for f in range(chunks):
            c_send[f, first:stop] = dot(weighted_onehot[span, :], emb[f]).reshape(
                stop - first, SLOTS, CHUNK
            )
            send(2, f, [p for p in order if first <= p < stop])
    for f in range(chunks):
        keep(2, f)

    def s_copy(off):
        return pltpu.make_async_remote_copy(
            src_ref=s_send,
            dst_ref=s_recv.at[off - 1],
            send_sem=s_ss,
            recv_sem=s_rs,
            device_id={"cls": lax.rem(mine + off, m)},
            device_id_type=pl.DeviceIdType.MESH,
        )

    for off in range(1, m):
        s_copy(off).start()
    pltpu.make_async_copy(s_recv, s_recv, s_rs).wait()
    full = s_send[...]
    for j in range(m - 1):
        full = full + s_recv[j]
    sim_ref[...] = full
    sim_copy = pltpu.make_async_copy(sim_ref, sim_out, out_sems.at[1])
    sim_copy.start()

    norm = jnp.zeros((CLS_PAD, 1), f32)
    for f in range(chunks):
        hi, lo = split(arrived(2, f))
        part = dot(to_classes, hi) + dot(to_classes, lo)
        own[f] = part
        norm = norm + jnp.sum(part * part, axis=1, keepdims=True)
    length = jnp.sqrt(norm + epsilon)
    for f in range(chunks):
        proto_ref[:, f * CHUNK : (f + 1) * CHUNK] = (own[f] / length)[:CLS_DEV, :]
    proto_copy = pltpu.make_async_copy(proto_ref, proto_out, out_sems.at[2])
    proto_copy.start()

    cnt_copy(1, n - 1).wait_send()
    for phase in range(3):
        for f in range(chunks):
            piece(phase, f, 0, 0, n).wait_send()
    pltpu.make_async_copy(s_recv, s_recv, s_ss).wait()
    for copy in (means_copy, sim_copy, proto_copy):
        copy.wait()


def finish(means_ref, proto_ref, sim_ref, means_out, proto_out, sim_out, sems):
    copies = [
        pltpu.make_async_copy(means_ref, means_out, sems.at[0]),
        pltpu.make_async_copy(proto_ref, proto_out, sems.at[1]),
        pltpu.make_async_copy(sim_ref, sim_out, sems.at[2]),
    ]
    for copy in copies:
        copy.start()
    for copy in copies:
        copy.wait()


def shards(embeddings, labels, row_count):
    rows, width = embeddings.shape
    n = lax.axis_size("dp")
    m = lax.axis_size("cls")
    chunks = width // CHUNK
    slots = n * SLOTS
    anywhere = pl.BlockSpec(memory_space=pl.ANY)
    exchange_buffer = pltpu.VMEM((chunks, n, SLOTS, CHUNK), f32)
    dma = pltpu.SemaphoreType.DMA
    results = (
        jax.ShapeDtypeStruct((CLS_DEV, width), f32),
        jax.ShapeDtypeStruct((CLS_DEV, width), f32),
        jax.ShapeDtypeStruct((1, rows), f32),
    )
    held = pl.pallas_call(
        functools.partial(kernel, n, m),
        out_shape=results,
        in_specs=[
            anywhere,
            pl.BlockSpec(memory_space=pltpu.HBM),
            pl.BlockSpec(memory_space=pltpu.HBM),
        ],
        out_specs=(anywhere,) * 3,
        scratch_shapes=[
            pltpu.SMEM((1,), jnp.int32),
            pltpu.VMEM((CLS_DEV, width), f32),
            pltpu.VMEM((CLS_DEV, width), f32),
            pltpu.VMEM((1, rows), f32),
            pltpu.VMEM((1, rows), jnp.int32),
            pltpu.VMEM((chunks, rows, CHUNK), bf16),
            pltpu.VMEM((slots, rows), bf16),
            pltpu.VMEM((slots, rows), bf16),
            pltpu.VMEM((slots, CLS_PAD), f32),
            pltpu.VMEM((n, 1, CLS_PAD), f32),
            pltpu.VMEM((n, 1, CLS_PAD), f32),
            exchange_buffer,
            exchange_buffer,
            exchange_buffer,
            exchange_buffer,
            exchange_buffer,
            exchange_buffer,
            pltpu.VMEM((1, rows), f32),
            pltpu.VMEM((m - 1, 1, rows), f32),
            pltpu.VMEM((1, rows), f32),
            pltpu.VMEM((1, rows), f32),
            pltpu.VMEM((chunks, CLS_PAD, CHUNK), f32),
            dma((3,)),
            dma,
            dma,
            dma((chunks,)),
            dma,
            dma,
            dma((3,)),
            dma((3, chunks, len(plan(n)[1]))),
            dma,
            dma,
        ],
        compiler_params=pltpu.CompilerParams(
            collective_id=0, has_side_effects=True, vmem_limit_bytes=32 * 1024 * 1024
        ),
    )(
        row_count,
        pltpu.with_memory_space_constraint(labels.reshape(1, rows), pltpu.HBM),
        pltpu.with_memory_space_constraint(embeddings, pltpu.HBM),
    )
    means, protos, similarity = pl.pallas_call(
        finish,
        out_shape=results,
        in_specs=[anywhere] * 3,
        out_specs=(anywhere,) * 3,
        scratch_shapes=[pltpu.SemaphoreType.DMA((3,))],
        compiler_params=pltpu.CompilerParams(vmem_limit_bytes=1024 * 1024),
    )(*held)
    return (means, protos, similarity.reshape(rows))


def solution(mesh):
    in_specs = (P("dp", None), P("dp"), P("dp"))
    out_specs = (P(("dp", "cls"), None), P(("dp", "cls"), None), P("dp"))
    return jax.shard_map(shards, mesh=mesh, in_specs=in_specs, out_specs=out_specs, check_vma=False)
```

```python
import functools

import jax
import jax.numpy as jnp
from jax import lax
from jax.experimental import pallas as pl
from jax.experimental.pallas import tpu as pltpu
from jax.sharding import PartitionSpec as P

CLS_DEV = 86
SLOTS = 16
CLS_PAD = 128
CHUNK = 384
ROW_TILE = 256

epsilon = 1e-06
sharpness = 4.0

f32 = jnp.float32
bf16 = jnp.bfloat16
NN = (((1,), (0,)), ((), ()))
NT = (((1,), (1,)), ((), ()))


def dot(a, b, dims=NN):
    return lax.dot_general(a, b, dims, preferred_element_type=f32)


def split(x):
    hi = x.astype(bf16)
    return hi, (x - hi.astype(f32)).astype(bf16)


def iota(shape, dim):
    return lax.broadcasted_iota(jnp.int32, shape, dim).astype(f32)


def plan(n):
    half = n // 2
    cut = max(1, half // 4)
    items = list(range(half)) + sorted(range(half, n), key=lambda k: (-(k // 2), k % 2))
    groups = [(0, half + cut), (half + cut, half + 2 * cut), (half + 2 * cut, n)]
    order = [half - 1] + list(range(half, n - 1)) + list(range(1, half - 1)) + [n - 1]
    return items, groups, order


def kernel(
    n,
    m,
    count_hbm,
    label_ref,
    emb_ref,
    means_out,
    proto_out,
    sim_out,
    count_ref,
    means_ref,
    proto_ref,
    sim_ref,
    label_rows,
    emb,
    onehot,
    weighted_onehot,
    place_t,
    cnt_send,
    cnt_recv,
    a_send,
    a_recv,
    b_send,
    b_recv,
    c_send,
    c_recv,
    s_send,
    s_recv,
    dot_row,
    len_row,
    own,
    out_sems,
    count_sem,
    label_sem,
    load_sem,
    cnt_ss,
    cnt_rs,
    big_ss,
    big_rs,
    s_ss,
    s_rs,
):
    rows = label_ref.shape[1]
    chunks = emb.shape[0]
    slots = n * SLOTS
    me = lax.axis_index("dp")
    mine = lax.axis_index("cls")
    items, groups, order = plan(n)

    def partner(p):
        target, bit = me, 1
        while bit < n:
            if items[p] & bit:
                target = target + bit - 2 * bit * lax.rem(lax.div(me, bit), 2)
            bit *= 2
        return target

    label_load = pltpu.make_async_copy(label_ref, label_rows, label_sem)
    label_load.start()
    count_load = pltpu.make_async_copy(count_hbm, count_ref, count_sem)
    count_load.start()
    barrier = pltpu.get_barrier_semaphore()
    for p in range(1, n):
        pl.semaphore_signal(
            barrier, inc=1, device_id={"dp": partner(p)}, device_id_type=pl.DeviceIdType.MESH
        )
    for off in range(1, m):
        pl.semaphore_signal(
            barrier, inc=1, device_id={"cls": lax.rem(mine + off, m)}, device_id_type=pl.DeviceIdType.MESH
        )
    loads = []
    for f in range(chunks):
        load = pltpu.make_async_copy(
            emb_ref.at[:, pl.ds(f * CHUNK, CHUNK)], emb.at[f], load_sem.at[f]
        )
        load.start()
        loads.append(load)

    position = lax.broadcasted_iota(jnp.int32, (n, rows), 0)
    peers = jnp.zeros((n, rows), f32)
    for p in range(n):
        peers = jnp.where(position == p, partner(p).astype(f32), peers)

    count_load.wait()
    label_load.wait()
    label = label_rows[...].astype(f32)
    block = jnp.floor((label + 0.5) * (1.0 / CLS_DEV))
    place = label - CLS_DEV * block
    owner = jnp.floor((block + 0.5) * (1.0 / m))
    group = block - m * owner
    alive = lax.broadcasted_iota(jnp.int32, (1, rows), 1) < count_ref[0]
    owned = (group == mine.astype(f32)) & alive
    place = jnp.where(owned, place, -1.0)
    owner = jnp.where(owned, owner, -1.0)

    owner_mask = peers == owner
    place_hot = jnp.where(iota((CLS_PAD, rows), 0) == place, 1.0, 0.0).astype(bf16)
    counts = dot(jnp.where(owner_mask, 1.0, 0.0).astype(bf16), place_hot, NT)
    upper = jnp.where(
        iota((CLS_PAD, CLS_PAD), 0) <= iota((CLS_PAD, CLS_PAD), 1), 1.0, 0.0
    ).astype(bf16)

    def ranks(table):
        return dot(jnp.where(table > 0, 1.0, 0.0).astype(bf16), upper) - 1.0

    for p in range(n):
        cnt_send[p] = counts[p : p + 1, :]
    cnt_recv[0] = cnt_send[0]

    rank_of = dot(ranks(counts).astype(bf16), place_hot) + SLOTS * iota((n, rows), 0)
    slot = jnp.sum(jnp.where(owner_mask, rank_of, 0.0), axis=0, keepdims=True)
    slot = jnp.where(owned, slot, -1.0)
    onehot[...] = jnp.where(iota((slots, rows), 0) == slot, 1.0, 0.0).astype(bf16)

    def dp_copy(p, src, dst, send_sem, recv_sem):
        return pltpu.make_async_remote_copy(
            src_ref=src,
            dst_ref=dst,
            send_sem=send_sem,
            recv_sem=recv_sem,
            device_id={"dp": partner(p)},
            device_id_type=pl.DeviceIdType.MESH,
        )

    def cnt_copy(p, count=1):
        span = pl.ds(p, count)
        return dp_copy(p, cnt_send.at[span], cnt_recv.at[span], cnt_ss, cnt_rs)

    buffers = ((a_send, a_recv), (b_send, b_recv), (c_send, c_recv))

    def big_copy(phase, f, p, g=0):
        out, recv = buffers[phase]
        return dp_copy(p, out.at[f, p], recv.at[f, p], big_ss.at[phase], big_rs.at[phase, f, g])

    def piece(phase, f, g, first, stop):
        out, recv = buffers[phase]
        span = pl.ds(max(first, 1), stop - max(first, 1))
        return dp_copy(
            max(first, 1), out.at[f, span], recv.at[f, span], big_ss.at[phase], big_rs.at[phase, f, g]
        )

    def send(phase, f, positions, g=0):
        for p in positions:
            if p > 0:
                big_copy(phase, f, p, g).start()

    def keep(phase, f):
        out, recv = buffers[phase]
        recv[f, 0] = out[f, 0]

    def arrived(phase, f, g=0, first=0, stop=n):
        piece(phase, f, g, first, stop).wait_recv()
        return buffers[phase][1][f, first:stop].reshape((stop - first) * SLOTS, CHUNK)

    loads[0].wait()
    a_send[0] = dot(onehot[...], emb[0]).reshape(n, SLOTS, CHUNK)
    pl.semaphore_wait(barrier, n - 1 + m - 1)
    for p in order:
        cnt_copy(p).start()
    send(0, 0, order)
    keep(0, 0)
    for f in range(1, chunks):
        loads[f].wait()

    for t in range(0, rows, ROW_TILE):
        squares = jnp.zeros((ROW_TILE, 128), f32)
        for f in range(chunks):
            for k in range(0, CHUNK, 128):
                x = emb[f, t : t + ROW_TILE, k : k + 128].astype(f32)
                squares = squares + x * x
        total = jnp.sum(jnp.transpose(squares), axis=0, keepdims=True)
        len_row[:, t : t + ROW_TILE] = jnp.sqrt(total + epsilon)

    for f in range(1, chunks):
        a_send[f] = dot(onehot[...], emb[f]).reshape(n, SLOTS, CHUNK)
        send(0, f, order)
        keep(0, f)

    cnt_copy(1, n - 1).wait_recv()
    table = jnp.concatenate([cnt_recv[p] for p in range(n)], axis=0)
    table_rank = jnp.where(table > 0, ranks(table), -1.0)
    slot_iota = iota((SLOTS, CLS_PAD), 0)
    for p in range(n):
        place_t[p * SLOTS : (p + 1) * SLOTS, :] = jnp.where(
            table_rank[p : p + 1, :] == slot_iota, 1.0, 0.0
        )
    to_slots = place_t[...].astype(bf16)
    to_classes = jnp.transpose(place_t[...]).astype(bf16)
    own_counts = jnp.maximum(jnp.sum(table, axis=0, keepdims=True), 1.0)
    divisor = jnp.transpose(jnp.broadcast_to(own_counts, (CLS_PAD, CLS_PAD)))[:, 0:1]

    for f in range(chunks):
        hi, lo = split(arrived(0, f))
        means = (dot(to_classes, hi) + dot(to_classes, lo)) / divisor
        hi, lo = split(means)
        b_send[f] = (dot(to_slots, hi) + dot(to_slots, lo)).reshape(n, SLOTS, CHUNK)
        for g, (first, stop) in enumerate(groups):
            send(1, f, [p for p in order if first <= p < stop], g)
        keep(1, f)
        means_ref[:, f * CHUNK : (f + 1) * CHUNK] = means[:CLS_DEV, :]
    means_copy = pltpu.make_async_copy(means_ref, means_out, out_sems.at[0])
    means_copy.start()

    def project(f, g, first, stop, start):
        mean = arrived(1, f, g, first, stop)
        height = (stop - first) * SLOTS
        both = jnp.concatenate(split(mean), axis=0)
        for t in range(0, rows, ROW_TILE):
            cols = slice(t, t + ROW_TILE)
            product = dot(both, emb[f, cols, :], NT)
            product = product[:height, :] + product[height:, :]
            hot = onehot[first * SLOTS : stop * SLOTS, cols].astype(f32)
            product = jnp.sum(product * hot, axis=0, keepdims=True)
            dot_row[:, cols] = product if start else dot_row[:, cols] + product
        return jnp.sum(mean * mean, axis=1, keepdims=True)

    norms = [0.0] * len(groups)
    for f in range(chunks - 1):
        for g, (first, stop) in enumerate(groups):
            norms[g] = norms[g] + project(f, g, first, stop, f == 0 and g == 0)
    for g, (first, stop) in enumerate(groups):
        span = slice(first * SLOTS, stop * SLOTS)
        norm = norms[g] + project(chunks - 1, g, first, stop, chunks == 1 and g == 0)
        scale = 1.0 / jnp.sqrt(norm + epsilon)
        for t in range(0, rows, ROW_TILE):
            cols = slice(t, t + ROW_TILE)
            hot = onehot[span, cols].astype(f32)
            row_scale = jnp.sum(hot * scale, axis=0, keepdims=True)
            similarity = dot_row[:, cols] * row_scale / len_row[:, cols]
            s_send[:, cols] = similarity if g == 0 else s_send[:, cols] + similarity
            weight = jnp.exp(sharpness * (similarity - 1.0))
            weighted_onehot[span, cols] = (hot * weight).astype(bf16)
        for f in range(chunks):
            c_send[f, first:stop] = dot(weighted_onehot[span, :], emb[f]).reshape(
                stop - first, SLOTS, CHUNK
            )
            send(2, f, [p for p in order if first <= p < stop])
    for f in range(chunks):
        keep(2, f)

    def s_copy(off):
        return pltpu.make_async_remote_copy(
            src_ref=s_send,
            dst_ref=s_recv.at[off - 1],
            send_sem=s_ss,
            recv_sem=s_rs,
            device_id={"cls": lax.rem(mine + off, m)},
            device_id_type=pl.DeviceIdType.MESH,
        )

    for off in range(1, m):
        s_copy(off).start()
    pltpu.make_async_copy(s_recv, s_recv, s_rs).wait()
    full = s_send[...]
    for j in range(m - 1):
        full = full + s_recv[j]
    sim_ref[...] = full
    sim_copy = pltpu.make_async_copy(sim_ref, sim_out, out_sems.at[1])
    sim_copy.start()

    norm = jnp.zeros((CLS_PAD, 1), f32)
    for f in range(chunks):
        hi, lo = split(arrived(2, f))
        part = dot(to_classes, hi) + dot(to_classes, lo)
        own[f] = part
        norm = norm + jnp.sum(part * part, axis=1, keepdims=True)
    length = jnp.sqrt(norm + epsilon)
    for f in range(chunks):
        proto_ref[:, f * CHUNK : (f + 1) * CHUNK] = (own[f] / length)[:CLS_DEV, :]
    proto_copy = pltpu.make_async_copy(proto_ref, proto_out, out_sems.at[2])
    proto_copy.start()

    cnt_copy(1, n - 1).wait_send()
    for phase in range(3):
        for f in range(chunks):
            piece(phase, f, 0, 0, n).wait_send()
    pltpu.make_async_copy(s_recv, s_recv, s_ss).wait()
    for copy in (means_copy, sim_copy, proto_copy):
        copy.wait()


def finish(means_ref, proto_ref, sim_ref, means_out, proto_out, sim_out, sems):
    copies = [
        pltpu.make_async_copy(means_ref, means_out, sems.at[0]),
        pltpu.make_async_copy(proto_ref, proto_out, sems.at[1]),
        pltpu.make_async_copy(sim_ref, sim_out, sems.at[2]),
    ]
    for copy in copies:
        copy.start()
    for copy in copies:
        copy.wait()


def shards(embeddings, labels, row_count):
    rows, width = embeddings.shape
    n = lax.axis_size("dp")
    m = lax.axis_size("cls")
    chunks = width // CHUNK
    slots = n * SLOTS
    anywhere = pl.BlockSpec(memory_space=pl.ANY)
    exchange_buffer = pltpu.VMEM((chunks, n, SLOTS, CHUNK), f32)
    dma = pltpu.SemaphoreType.DMA
    results = (
        jax.ShapeDtypeStruct((CLS_DEV, width), f32),
        jax.ShapeDtypeStruct((CLS_DEV, width), f32),
        jax.ShapeDtypeStruct((1, rows), f32),
    )
    held = pl.pallas_call(
        functools.partial(kernel, n, m),
        out_shape=results,
        in_specs=[
            anywhere,
            pl.BlockSpec(memory_space=pltpu.HBM),
            pl.BlockSpec(memory_space=pltpu.HBM),
        ],
        out_specs=(anywhere,) * 3,
        scratch_shapes=[
            pltpu.SMEM((1,), jnp.int32),
            pltpu.VMEM((CLS_DEV, width), f32),
            pltpu.VMEM((CLS_DEV, width), f32),
            pltpu.VMEM((1, rows), f32),
            pltpu.VMEM((1, rows), jnp.int32),
            pltpu.VMEM((chunks, rows, CHUNK), bf16),
            pltpu.VMEM((slots, rows), bf16),
            pltpu.VMEM((slots, rows), bf16),
            pltpu.VMEM((slots, CLS_PAD), f32),
            pltpu.VMEM((n, 1, CLS_PAD), f32),
            pltpu.VMEM((n, 1, CLS_PAD), f32),
            exchange_buffer,
            exchange_buffer,
            exchange_buffer,
            exchange_buffer,
            exchange_buffer,
            exchange_buffer,
            pltpu.VMEM((1, rows), f32),
            pltpu.VMEM((m - 1, 1, rows), f32),
            pltpu.VMEM((1, rows), f32),
            pltpu.VMEM((1, rows), f32),
            pltpu.VMEM((chunks, CLS_PAD, CHUNK), f32),
            dma((3,)),
            dma,
            dma,
            dma((chunks,)),
            dma,
            dma,
            dma((3,)),
            dma((3, chunks, len(plan(n)[1]))),
            dma,
            dma,
        ],
        compiler_params=pltpu.CompilerParams(
            collective_id=0, has_side_effects=True, vmem_limit_bytes=32 * 1024 * 1024
        ),
    )(
        row_count,
        pltpu.with_memory_space_constraint(labels.reshape(1, rows), pltpu.HBM),
        pltpu.with_memory_space_constraint(embeddings, pltpu.HBM),
    )
    means, protos, similarity = pl.pallas_call(
        finish,
        out_shape=results,
        in_specs=[anywhere] * 3,
        out_specs=(anywhere,) * 3,
        scratch_shapes=[pltpu.SemaphoreType.DMA((3,))],
        compiler_params=pltpu.CompilerParams(vmem_limit_bytes=1024 * 1024),
    )(*held)
    return (means, protos, similarity.reshape(rows))


def solution(mesh):
    in_specs = (P("dp", None), P("dp"), P("dp"))
    out_specs = (P(("dp", "cls"), None), P(("dp", "cls"), None), P("dp"))
    return jax.shard_map(shards, mesh=mesh, in_specs=in_specs, out_specs=out_specs, check_vma=False)
```
